32 devices in a mesh: space: 16 (over z, y, core), tensor: 2 (over x).
Axes of the slice: x: 2, y: 2, z: 4, core: 2. Of those that a mesh axis runs over, the one named last changes fastest.
Arguments:
- tokens: bfloat16 [14336, 1024], P('space', 'tensor'), may hold values from -6 to 6
- first_weight: bfloat16 [1024, 1024], P(None, 'tensor'), may hold values from -0.1875 to 0.1875
- second_weight: bfloat16 [1024, 1024], P(None, 'tensor'), may hold values from -0.1875 to 0.1875
- head_weight: bfloat16 [352, 1024], P('tensor'), may hold values from -0.1875 to 0.1875
- targets: float32 [352, 14336], P('tensor', 'space'), may hold values from -6 to 6
- land_mask: int32 [4, 14336], P(None, 'space'), may hold values from 0 to 1, as said below
- variable_kind: int32 [88], P('tensor'), may hold values from 0 to 2
- loss_scale: float32 [], replicated, may hold values from 630784 to 5046272
Outputs:
- loss: float32 [], replicated
- token_grad: float32 [14336, 1024], P('space', 'tensor')
- first_grad: float32 [1024, 1024], P('space', 'tensor')
- second_grad: float32 [1024, 1024], P('space', 'tensor')
- head_grad: float32 [352, 1024], P('tensor', 'space')
The draws below stay inside these ranges and needn't reach their ends.
Inputs may be any that keep to these rules, and one draw needn't show every extreme that they name: `land_mask`: every aligned group of 8 entries along the last dimension holds at least one 1 and one 0. `variable_kind`: 0 scores a variable on all cells, 1 on land cells, 2 on ocean cells.
All inputs are finite; a program needn't handle non-finite values.
Results may differ from the reference program's by a relative error of at most 0.0056.
Values may be sent and summed in bfloat16 or wider, within the bound.
A program may use at most 64 MiB of HBM per device.

```python
import math
import jax
import jax.numpy as jnp
from jax import lax

D = 1024
V = 88
PP = 4
LONP = 224
TOKENS = 14336
COLS = 352


def draw_land_mask(key, part):
    level_key = jax.random.fold_in(key, 21)
    band_key = jax.random.fold_in(key, 22)
    sector_key = jax.random.fold_in(key, 23)
    cell_key = jax.random.fold_in(key, 24)
    first = jax.random.fold_in(key, 25)
    second = jax.random.fold_in(key, 26)
    low_level = jax.random.randint(jax.random.fold_in(level_key, 1), (), 4, 21)
    high_level = jax.random.randint(jax.random.fold_in(level_key, 2), (), 55, 76)
    picker = jax.random.randint(jax.random.fold_in(level_key, 3), (), 0, 2)
    level = jnp.where(picker == 0, low_level, high_level).astype(jnp.int32)
    band_count = TOKENS // LONP
    band_shift = jax.random.randint(band_key, (band_count,), -25, 26).astype(jnp.int32)
    sector_shift = jax.random.randint(sector_key, (8,), -15, 16).astype(jnp.int32)
    position = jnp.arange(TOKENS, dtype=jnp.int32)
    band_index = position // LONP
    sector_index = position % LONP // (LONP // 8)
    chance = jnp.clip(level + band_shift[band_index] + sector_shift[sector_index], 2, 95).astype(jnp.int32)
    rolled = jax.random.randint(cell_key, (PP, TOKENS), 0, 100).astype(jnp.int32)
    base = (rolled < chance[None, :]).astype(jnp.int32)
    blocks = TOKENS // 8
    base = base.reshape(PP, blocks, 8)
    where_one = jax.random.randint(first, (PP, blocks, 1), 0, 8).astype(jnp.int32)
    where_zero = (where_one + jax.random.randint(second, (PP, blocks, 1), 1, 8).astype(jnp.int32)) % 8
    places = jnp.arange(8, dtype=jnp.int32)[None, None, :]
    base = jnp.where(places == where_one, 1, base)
    base = jnp.where(places == where_zero, 0, base)
    return base.reshape(PP, TOKENS).astype(jnp.int32)


def with_ends(array, key, low, high):
    shape = array.shape
    place = [jax.random.randint(jax.random.fold_in(key, axis), (), 0, shape[axis]) for axis in range(len(shape))]
    array = array.at[tuple(place)].set(low)
    longest = shape.index(max(shape))
    place[longest] = (place[longest] + 1) % shape[longest]
    return array.at[tuple(place)].set(high)


def raised(entries, own_key, source, target, parts, factor):
    def block_of(dim):
        return (jnp.arange(entries.shape[dim]) // (entries.shape[dim] // parts)).reshape((-1,) + (1,) * (entries.ndim - 1 - dim))

    one_side = jax.random.permutation(own_key, parts)[block_of(target)]
    second = (block_of(target) + parts // 2) % parts
    return jnp.where((block_of(source) == one_side) | (block_of(source) == second), factor * entries, entries)


def block_levels(key, extent, cuts, smallest, high):
    def one(dim, blocks):
        steps = jax.random.uniform(jax.random.fold_in(jax.random.fold_in(key, 6), dim), (blocks,), jnp.float32, smallest / len(cuts), high / len(cuts))
        return jnp.repeat(jnp.exp(steps), extent[dim] // blocks).reshape((-1,) + (1,) * (len(extent) - dim - 1))

    gain = one(*cuts[0])
    for cut in cuts[1:]:
        gain = gain * one(*cut)
    return gain


def gaussian(stream_key, extent, spread, reach, cuts=(), kind=jnp.bfloat16):
    level = block_levels(stream_key, extent, cuts, -0.22, 0.18) if cuts else 1.0
    drawn = jax.random.normal(stream_key, extent, jnp.float32) * spread * level
    return jnp.minimum(jnp.maximum(drawn, -reach), reach).astype(kind)


def bell_draw_with(key, shape, scale, limit, split, heavy, held_as=jnp.bfloat16):
    values = scale * jax.random.normal(key, shape, jnp.float32)
    if split:
        values = values * block_levels(key, shape, split, -0.22, 0.18)
    return jnp.clip(raised(values, jax.random.fold_in(key, 3), *heavy), -limit, limit).astype(held_as)


def setup_inputs(seed: int = 0) -> dict:
    keys = jax.random.split(jax.random.key(seed), 9)
    return {
        "tokens": bell_draw_with(keys[0], (TOKENS, D), 1.0, 6.0, ((0, 16), (1, 2)), (0, 1, 16, 2.0)),
        "first_weight": gaussian(keys[1], (D, D), D ** -0.5, 0.1875, ((1, 2),)),
        "second_weight": gaussian(keys[2], (D, D), D ** -0.5, 0.1875, ((1, 2),)),
        "head_weight": gaussian(keys[3], (COLS, D), D ** -0.5, 0.1875, ((0, 2),)),
        "targets": gaussian(keys[4], (COLS, TOKENS), 1.0, 6.0, ((0, 2), (1, 16)), jnp.float32),
        "land_mask": draw_land_mask(jax.random.fold_in(keys[8], 71), 0),
        "variable_kind": with_ends(jax.random.randint(keys[6], (V,), 0, 3), jax.random.fold_in(keys[6], 1), 0, 2).astype(jnp.int32),
        "loss_scale": jnp.clip(jnp.exp(jax.random.uniform(keys[7], (), jnp.float32, math.log(630784.0), math.log(5046272))), 630784.0, 5046272),
    }


def slope(z):
    cdf = 0.5 * (1.0 + lax.erf(z / math.sqrt(2.0)))
    return cdf + z * jnp.exp(-0.5 * z * z) / math.sqrt(2.0 * math.pi)

def reference(tokens, first_weight, second_weight, head_weight, targets, land_mask, variable_kind, loss_scale):
    pre_one = jnp.dot(tokens, first_weight, preferred_element_type=jnp.float32)
    hidden_one = jax.nn.gelu(pre_one, approximate=False).astype(jnp.bfloat16)
    pre_two = jnp.dot(hidden_one, second_weight, preferred_element_type=jnp.float32)
    hidden_two = jax.nn.gelu(pre_two, approximate=False).astype(jnp.bfloat16)
    predicted = jnp.dot(head_weight, hidden_two.T, preferred_element_type=jnp.float32)
    position = jnp.arange(TOKENS, dtype=jnp.int32)
    cell = jnp.arange(PP, dtype=jnp.int32)
    lat_row = 2 * (position // LONP)[None, :] + (cell // 2)[:, None]
    nlat = 2 * TOKENS // LONP
    cell_weight = jnp.cos(math.pi / 2.0 * (lat_row.astype(jnp.float32) + 0.5) / nlat)
    land = land_mask.astype(jnp.float32)
    kind = variable_kind[:, None, None]
    valid = jnp.where(kind == 0, 1.0, jnp.where(kind == 1, land[None], 1.0 - land[None])).astype(jnp.float32)
    masked = cell_weight[None] * valid
    error = predicted.reshape(V, PP, TOKENS) - targets.reshape(V, PP, TOKENS)
    weight_sum = lax.optimization_barrier(jnp.sum(masked, axis=(1, 2)))
    error_sum = lax.optimization_barrier(jnp.sum(masked * error * error, axis=(1, 2)))
    root = jnp.sqrt(error_sum / weight_sum + 1e-06)
    loss = jnp.mean(root)
    coef = loss_scale / (V * root * weight_sum)
    grad_pred = (coef[:, None, None] * masked * error).reshape(COLS, TOKENS).astype(jnp.bfloat16)
    head_grad = jnp.dot(grad_pred, hidden_two, preferred_element_type=jnp.float32)
    back_two = jnp.dot(grad_pred.T, head_weight, preferred_element_type=jnp.float32)
    grad_two = (back_two * slope(pre_two)).astype(jnp.bfloat16)
    second_grad = jnp.dot(hidden_one.T, grad_two, preferred_element_type=jnp.float32)
    back_one = jnp.dot(grad_two, second_weight.T, preferred_element_type=jnp.float32)
    grad_one = (back_one * slope(pre_one)).astype(jnp.bfloat16)
    first_grad = jnp.dot(tokens.T, grad_one, preferred_element_type=jnp.float32)
    token_grad = jnp.dot(grad_one, first_weight.T, preferred_element_type=jnp.float32)
    return (loss, token_grad, first_grad, second_grad, head_grad)
```

```python
import functools
import math

import jax
import jax.numpy as jnp
from jax import lax
from jax.experimental import pallas as pl
from jax.experimental.pallas import tpu as pltpu
from jax.sharding import PartitionSpec as P

PP = 4
PROW_DEV = 4
LONP = 224
MESH = pl.DeviceIdType.MESH
VMEM = pl.BlockSpec(memory_space=pltpu.VMEM)


def slope(z):
    cdf = 0.5 * (1.0 + lax.erf(z / math.sqrt(2.0)))
    return cdf + z * jnp.exp(-0.5 * z * z) / math.sqrt(2.0 * math.pi)


def flipped(s, bit):
    step = 1 << bit
    return s + step - 2 * step * ((s // step) % 2)


def greet(partners):
    barrier = pltpu.get_barrier_semaphore()
    for partner in partners:
        pl.semaphore_signal(barrier, inc=1, device_id=partner, device_id_type=MESH)
    pl.semaphore_wait(barrier, len(partners))


def params(number):
    return pltpu.CompilerParams(
        collective_id=number, has_side_effects=True, vmem_limit_bytes=60 * 2**20
    )


def gather_kernel(
    tok, one, two, head, tar, o_tok, o_one, o_two, o_head, o_tar, send, recv, local
):
    s, x = lax.axis_index("space"), lax.axis_index("tensor")
    other = 1 - x
    across, core, along = (s, other), (flipped(s, 0), x), (flipped(s, 1), x)
    quarter = s % 4
    beyond = (quarter + 2) % 4
    width = one.shape[1]
    rows = one.shape[0] // 4
    cols = head.shape[1] // 4
    half = o_tok.shape[0]

    def span(index, size):
        return pl.ds(pl.multiple_of(index * size, size), size)

    sources = [
        one.at[span(quarter, rows), :],
        two.at[span(quarter, rows), :],
        head.at[:, span(quarter, cols)],
    ]
    places = [
        lambda side, q: o_one.at[span(q, rows), span(side, width)],
        lambda side, q: o_two.at[span(q, rows), span(side, width)],
        lambda side, q: o_head.at[side, :, span(q, cols)],
    ]

    greet([across, core, along])

    def remote(src, dst, slot, target):
        copy = pltpu.make_async_remote_copy(
            src_ref=src,
            dst_ref=dst,
            send_sem=send.at[slot],
            recv_sem=recv.at[slot],
            device_id=target,
            device_id_type=MESH,
        )
        copy.start()
        return copy

    firsts = [remote(sources[k], places[k](x, quarter), k, across) for k in range(3)]
    extra = [
        remote(tok.at[span(other, half), :], o_tok.at[:, span(x, width)], 12, across),
        remote(tar.at[other], o_tar.at[x], 13, across),
    ]
    own = [
        pltpu.make_async_copy(one, o_one.at[:, span(x, width)], local.at[0]),
        pltpu.make_async_copy(two, o_two.at[:, span(x, width)], local.at[1]),
        pltpu.make_async_copy(head, o_head.at[x], local.at[2]),
        pltpu.make_async_copy(tok.at[span(x, half), :], o_tok.at[:, span(x, width)], local.at[3]),
        pltpu.make_async_copy(tar.at[x], o_tar.at[x], local.at[4]),
    ]
    for copy in own:
        copy.start()
    cores, alongs, lasts = [], [], []

    def forward(k):
        firsts[k].wait_recv()
        piece = places[k](other, quarter)
        alongs.append(remote(piece, piece, 3 + k, along))
        cores.append(remote(piece, piece, 6 + k, core))

    def finish(k):
        alongs[k].wait_recv()
        piece = places[k](other, beyond)
        lasts.append(remote(piece, piece, 9 + k, core))

    forward(0)
    forward(1)
    finish(0)
    forward(2)
    finish(1)
    finish(2)
    for copy in cores + lasts + extra:
        copy.wait_recv()
    for copy in firsts + alongs + cores + lasts + extra:
        copy.wait_send()
    for copy in own:
        copy.wait()


def gather(tokens, first, second, head, targets):
    count, width = tokens.shape
    half = count // 2
    shape = jax.ShapeDtypeStruct
    return pl.pallas_call(
        gather_kernel,
        out_shape=(
            shape((half, 2 * width), tokens.dtype),
            shape((first.shape[0], 2 * first.shape[1]), first.dtype),
            shape((second.shape[0], 2 * second.shape[1]), second.dtype),
            shape((2,) + head.shape, head.dtype),
            shape(targets.shape, targets.dtype),
        ),
        in_specs=[VMEM] * 5,
        out_specs=[VMEM] * 5,
        scratch_shapes=[
            pltpu.SemaphoreType.DMA((14,)),
            pltpu.SemaphoreType.DMA((14,)),
            pltpu.SemaphoreType.DMA((5,)),
        ],
        compiler_params=params(0),
        name="gather",
    )(tokens, first, second, head, targets)


def total_kernel(groups, v_ref, o_ref, near, far, mid, send, recv):
    s, x = lax.axis_index("space"), lax.axis_index("tensor")
    low, high = s % 4, s // 4
    mine = x * 4 + low

    def near_peer(d):
        j = (mine + d) % 8
        return (high * 4 + j % 4, j // 4)

    def far_peer(d):
        return (((high + d) % groups) * 4 + low, x)

    greet([near_peer(d) for d in range(1, 8)] + [far_peer(d) for d in range(1, groups)])

    def share(src, slots, me, peers, base):
        copies = []
        for n, peer in enumerate(peers):
            copy = pltpu.make_async_remote_copy(
                src_ref=src,
                dst_ref=slots.at[me],
                send_sem=send.at[base + n],
                recv_sem=recv.at[base + n],
                device_id=peer,
                device_id_type=MESH,
            )
            copy.start()
            copies.append(copy)
        slots[me] = src[...]
        for copy in copies:
            copy.wait()

    share(v_ref, near, mine, [near_peer(d) for d in range(1, 8)], 0)
    mid[...] = jnp.sum(near[...], axis=0)
    share(mid, far, high, [far_peer(d) for d in range(1, groups)], 7)
    o_ref[...] = jnp.sum(far[...], axis=0)


def total(values):
    groups = lax.axis_size("space") // 4
    return pl.pallas_call(
        functools.partial(total_kernel, groups),
        out_shape=jax.ShapeDtypeStruct(values.shape, values.dtype),
        in_specs=[VMEM],
        out_specs=VMEM,
        scratch_shapes=[
            pltpu.VMEM((8,) + values.shape, values.dtype),
            pltpu.VMEM((groups,) + values.shape, values.dtype),
            pltpu.VMEM(values.shape, values.dtype),
            pltpu.SemaphoreType.DMA((6 + groups,)),
            pltpu.SemaphoreType.DMA((6 + groups,)),
        ],
        compiler_params=params(1),
        name="total",
    )(values)


X = -1


def orders(bits):
    rest = list(range(3, bits))
    return ([0, 1, 2, X] + rest, [0, 2, 1, X] + rest, [0, X, 1, 2] + rest)


def pieces(bits, order, shape):
    found = []
    left = list(range(bits))[::-1]
    rows, cols = shape
    for bit in order:
        if bit == X:
            cols //= 2
        else:
            left.remove(bit)
        found.append((2,) * len(left) + (rows, cols))
    return found


def scatter_kernel(bits, steps, *refs):
    (g_one, g_two, g_head, tok), refs = refs[:4], refs[4:]
    (outs, o_tok), refs = (refs[:3], refs[3]), refs[4:]
    count = bits + 1
    landing = [refs[count * k : count * (k + 1)] for k in range(3)]
    refs = refs[3 * count :]
    kept = [refs[bits * k : bits * (k + 1)] for k in range(3)]
    send, recv = refs[3 * bits :]
    s, x = lax.axis_index("space"), lax.axis_index("tensor")

    def peer(bit):
        return (s, 1 - x) if bit == X else (flipped(s, bit), x)

    def part(ref, left, bit, near):
        if bit == X:
            width = ref.shape[-1] // 2
            side = x if near else 1 - x
            place = pl.ds(pl.multiple_of(side * width, width), width)
            return (slice(None),) * (len(ref.shape) - 1) + (place,)
        value = (s // (1 << bit)) % 2
        value = value if near else 1 - value
        return (slice(None),) * left.index(bit) + (value,)

    greet([peer(b) for b in [X] + list(range(bits))])

    def start(k, n, ref, left):
        bit = steps[k][n]
        copy = pltpu.make_async_remote_copy(
            src_ref=ref.at[part(ref, left, bit, False)],
            dst_ref=landing[k][n],
            send_sem=send.at[k * count + n],
            recv_sem=recv.at[k * count + n],
            device_id=peer(bit),
            device_id_type=MESH,
        )
        copy.start()
        return copy

    state = []
    for k, ref in ((1, g_two), (0, g_one), (2, g_head)):
        left = list(range(bits))[::-1]
        state.append([k, ref, left, start(k, 0, ref, left)])
    width = tok.shape[1] // 2
    tail = pltpu.make_async_remote_copy(
        src_ref=tok.at[:, pl.ds(pl.multiple_of((1 - x) * width, width), width)],
        dst_ref=o_tok,
        send_sem=send.at[3 * count],
        recv_sem=recv.at[3 * count],
        device_id=peer(X),
        device_id_type=MESH,
    )
    tail.start()
    copies = [tail]
    for n in range(count):
        for entry in state:
            k, ref, left, copy = entry
            bit = steps[k][n]
            copies.append(copy)
            copy.wait_recv()
            mine = ref[part(ref, left, bit, True)].astype(jnp.float32)
            both = mine + landing[k][n][...].astype(jnp.float32)
            if n == count - 1:
                outs[k][...] = both
                continue
            target = kept[k][n]
            target[...] = both.astype(target.dtype)
            left = [b for b in left if b != bit]
            entry[1:] = [target, left, start(k, n + 1, target, left)]
    tail.wait_recv()
    for copy in copies:
        copy.wait_send()


def scatter(g_one, g_two, g_head, tok):
    size = lax.axis_size("space")
    bits = size.bit_length() - 1
    steps = orders(bits)
    inputs = [g.reshape((2,) * bits + (g.shape[0] // size, g.shape[1])) for g in (g_one, g_two, g_head)]
    shapes = [pieces(bits, steps[k], inputs[k].shape[-2:]) for k in range(3)]
    low = jnp.bfloat16
    scratch = [pltpu.VMEM(shape, low) for k in range(3) for shape in shapes[k]]
    scratch += [pltpu.VMEM(shape, low) for k in range(3) for shape in shapes[k][:-1]]
    slots = 3 * (bits + 1) + 1
    return pl.pallas_call(
        functools.partial(scatter_kernel, bits, steps),
        out_shape=tuple(jax.ShapeDtypeStruct(shapes[k][-1], jnp.float32) for k in range(3))
        + (jax.ShapeDtypeStruct((tok.shape[0], tok.shape[1] // 2), tok.dtype),),
        in_specs=[VMEM] * 4,
        out_specs=[VMEM] * 4,
        scratch_shapes=scratch
        + [pltpu.SemaphoreType.DMA((slots,)), pltpu.SemaphoreType.DMA((slots,))],
        compiler_params=params(2),
        name="scatter",
    )(*inputs, tok)


def mix(a, b, dims):
    return lax.dot_general(a, b, ((dims[:1], dims[1:]), ((), ())), preferred_element_type=jnp.float32)


def per_device(
    tokens, first_weight, second_weight, head_weight, targets, land_mask, variable_kind, loss_scale
):
    low = jnp.bfloat16
    count, width = tokens.shape
    half = count // 2
    rows = head_weight.shape[0]
    kinds = 2 * rows // PP
    s, x = lax.axis_index("space"), lax.axis_index("tensor")
    lanes = -(-(half + 1) // 128) * 128
    sent = jnp.stack([targets[:, :half], targets[:, half:]]).astype(low)
    label = jnp.repeat(variable_kind, PP).astype(low)[None, :, None]
    label = jnp.broadcast_to(label, (2, rows, lanes - half))
    sent = jnp.concatenate([sent, label], axis=2)
    toks, w_one, w_two, w_head, seen = gather(
        tokens, first_weight, second_weight, head_weight, sent
    )
    w_head = w_head.reshape(2 * rows, -1)
    goal = seen[:, :, :half].reshape(kinds, PP, half)
    kind = seen[:, :, half].reshape(kinds, PP)[:, :, None]

    position = s * count + x * half + jnp.arange(half, dtype=jnp.int32)
    cell = jnp.arange(PP, dtype=jnp.int32)
    lat_row = 2 * (position // LONP)[None, :] + (cell // 2)[:, None]
    nlat = 2 * PROW_DEV * lax.axis_size("space")
    cell_weight = jnp.cos(math.pi / 2.0 * (lat_row.astype(jnp.float32) + 0.5) / nlat)
    land = lax.dynamic_slice_in_dim(land_mask, x * half, half, 1).astype(jnp.float32)
    valid = jnp.where(kind == 0, 1.0, jnp.where(kind == 1, land[None], 1.0 - land[None]))
    masked = cell_weight[None] * valid

    pre_one = mix(toks, w_one, (1, 0))
    hidden_one = jax.nn.gelu(pre_one, approximate=False).astype(low)
    pre_two = mix(hidden_one, w_two, (1, 0))
    hidden_two = jax.nn.gelu(pre_two, approximate=False).astype(low)
    predicted = mix(w_head, hidden_two, (1, 1))
    error = predicted.reshape(kinds, PP, half) - goal.astype(jnp.float32)
    scored = masked * error
    sums = jnp.stack([jnp.sum(scored * error, axis=(1, 2)), jnp.sum(masked, axis=(1, 2))])
    wide = -(-kinds // 128) * 128
    sums = total(jnp.pad(sums, ((0, 6), (0, wide - kinds))))
    weight_sum = sums[1, :kinds]
    root = jnp.sqrt(sums[0, :kinds] / weight_sum + 1e-06)
    loss = jnp.sum(root) / kinds
    coef = loss_scale / (kinds * root * weight_sum)
    grad_pred = (coef[:, None, None] * scored).reshape(kinds * PP, half).astype(low)

    head_term = mix(hidden_two, grad_pred, (0, 1)).astype(low)
    pad = jnp.zeros((head_term.shape[0], -rows % 128), low)
    head_term = jnp.concatenate([head_term[:, :rows], pad, head_term[:, rows:], pad], axis=1)
    grad_two = (mix(grad_pred, w_head, (0, 0)) * slope(pre_two)).astype(low)
    second_term = mix(hidden_one, grad_two, (0, 0)).astype(low)
    grad_one = (mix(grad_two, w_two, (1, 1)) * slope(pre_one)).astype(low)
    first_term = mix(toks, grad_one, (0, 0)).astype(low)
    token_term = mix(grad_one, w_one, (1, 1)).astype(low)
    first_grad, second_grad, head_grad, arrived = scatter(
        first_term, second_term, head_term, token_term
    )
    kept = lax.dynamic_slice_in_dim(token_term, x * width, width, 1)
    upper = jnp.where(x == 0, kept, arrived)
    lower = jnp.where(x == 0, arrived, kept)
    token_grad = jnp.concatenate([upper, lower], axis=0).astype(jnp.float32)
    return (loss, token_grad, first_grad, second_grad, head_grad[:, :rows].T)


def column_folder(weights, piece):
    return lax.dot_general(
        piece, weights, (((1,), (1,)), ((), ())), preferred_element_type=jnp.float32
    )


def row_folder(weights, piece):
    return lax.dot_general(
        piece, weights, (((0,), (0,)), ((), ())), preferred_element_type=jnp.float32
    )


def per_device_wide(
    tokens, first_weight, second_weight, head_weight, targets, land_mask, variable_kind, loss_scale
):
    count = tokens.shape[0]
    width = first_weight.shape[1]
    kinds = head_weight.shape[0] // PP
    rows_first, rows_second = (
        lax.all_to_all(first_weight, "tensor", split_axis=0, concat_axis=1, tiled=True),
        lax.all_to_all(second_weight, "tensor", split_axis=0, concat_axis=1, tiled=True),
    )
    head_cols = lax.all_to_all(head_weight, "tensor", split_axis=1, concat_axis=0, tiled=True)
    position = lax.axis_index("space") * count + jnp.arange(count, dtype=jnp.int32)
    cell = jnp.arange(PP, dtype=jnp.int32)
    lat_row = 2 * (position // LONP)[None, :] + (cell // 2)[:, None]
    nlat = 2 * PROW_DEV * lax.axis_size("space")
    cell_weight = jnp.cos(math.pi / 2.0 * (lat_row.astype(jnp.float32) + 0.5) / nlat)
    land = land_mask.astype(jnp.float32)
    kind = variable_kind[:, None, None]
    valid = jnp.where(kind == 0, 1.0, jnp.where(kind == 1, land[None], 1.0 - land[None]))
    masked = cell_weight[None] * valid
    local_weight = jnp.sum(masked, axis=(1, 2))
    weight_sum = lax.psum(local_weight, "space")
    full_in = lax.all_gather(tokens, "tensor", axis=1, tiled=True)
    pre_one = jnp.dot(full_in, first_weight, preferred_element_type=jnp.float32)
    hidden_one = jax.nn.gelu(pre_one, approximate=False).astype(jnp.bfloat16)
    full_one = lax.all_gather(hidden_one, "tensor", axis=1, tiled=True)
    pre_two = jnp.dot(full_one, second_weight, preferred_element_type=jnp.float32)
    hidden_two = jax.nn.gelu(pre_two, approximate=False).astype(jnp.bfloat16)
    full_two = lax.all_gather(hidden_two, "tensor", axis=1, tiled=True)
    predicted = lax.dot_general(
        head_weight, full_two, (((1,), (1,)), ((), ())), preferred_element_type=jnp.float32
    )
    error = predicted.reshape(kinds, PP, count) - targets.reshape(kinds, PP, count)
    local_error = jnp.sum(masked * error * error, axis=(1, 2))
    error_sum = lax.psum(local_error, "space")
    root = jnp.sqrt(error_sum / weight_sum + 1e-06)
    loss = lax.psum(jnp.sum(root), "tensor") / (kinds * lax.axis_size("tensor"))
    coef = loss_scale / (kinds * lax.axis_size("tensor") * root * weight_sum)
    grad_pred = (
        (coef[:, None, None] * masked * error).reshape(kinds * PP, count).astype(jnp.bfloat16)
    )
    back_two = row_folder(head_cols, lax.all_gather(grad_pred, "tensor", axis=0, tiled=True))
    head_term = jnp.dot(grad_pred, full_two, preferred_element_type=jnp.float32)
    head_grad = lax.psum_scatter(head_term, "space", scatter_dimension=1, tiled=True)
    grad_two = (back_two * slope(pre_two)).astype(jnp.bfloat16)
    back_one = column_folder(rows_second, lax.all_gather(grad_two, "tensor", axis=1, tiled=True))
    grad_one = (back_one * slope(pre_one)).astype(jnp.bfloat16)
    joined = lax.psum_scatter(
        jnp.concatenate(
            [
                lax.dot_general(
                    full_one, grad_two, (((0,), (0,)), ((), ())), preferred_element_type=jnp.float32
                ),
                lax.dot_general(
                    full_in, grad_one, (((0,), (0,)), ((), ())), preferred_element_type=jnp.float32
                ),
            ],
            axis=1,
        ),
        "space",
        scatter_dimension=0,
        tiled=True,
    )
    second_grad = joined[:, :width]
    first_grad = joined[:, width:]
    token_grad = column_folder(rows_first, lax.all_gather(grad_one, "tensor", axis=1, tiled=True))
    return (loss, token_grad, first_grad, second_grad, head_grad)


def solution(mesh):
    size = mesh.shape["space"]
    paired = mesh.shape["tensor"] == 2 and size >= 8 and size & (size - 1) == 0
    return jax.shard_map(
        per_device if paired else per_device_wide,
        mesh=mesh,
        in_specs=(
            P("space", "tensor"),
            P(None, "tensor"),
            P(None, "tensor"),
            P("tensor", None),
            P("tensor", "space"),
            P(None, "space"),
            P("tensor"),
            P(),
        ),
        out_specs=(
            P(),
            P("space", "tensor"),
            P("space", "tensor"),
            P("space", "tensor"),
            P("tensor", "space"),
        ),
        check_vma=False,
    )
```

```python
import functools
import math

import jax
import jax.numpy as jnp
from jax import lax
from jax.experimental import pallas as pl
from jax.experimental.pallas import tpu as pltpu
from jax.sharding import PartitionSpec as P

PP = 4
PROW_DEV = 4
LONP = 224
MESH = pl.DeviceIdType.MESH
VMEM = pl.BlockSpec(memory_space=pltpu.VMEM)


def bent(z):
    return (0.5 * z * (1.0 + lax.erf(z / math.sqrt(2.0)))).astype(jnp.bfloat16)


def slope(z):
    cdf = 0.5 * (1.0 + lax.erf(z / math.sqrt(2.0)))
    return cdf + z * jnp.exp(-0.5 * z * z) / math.sqrt(2.0 * math.pi)


def flipped(s, bit):
    step = 1 << bit
    return s + step - 2 * step * ((s // step) % 2)


def greet(partners):
    barrier = pltpu.get_barrier_semaphore()
    for partner in partners:
        pl.semaphore_signal(barrier, inc=1, device_id=partner, device_id_type=MESH)
    pl.semaphore_wait(barrier, len(partners))


def params(number):
    return pltpu.CompilerParams(
        collective_id=number, has_side_effects=True, vmem_limit_bytes=60 * 2**20
    )


def gather_kernel(
    tok, one, two, head, tar, o_tok, o_one, o_two, o_head, o_tar, send, recv, local
):
    s, x = lax.axis_index("space"), lax.axis_index("tensor")
    other = 1 - x
    across, core, along, up = (s, other), (flipped(s, 0), x), (flipped(s, 1), x), (flipped(s, 2), x)
    mine = s % 8
    width = one.shape[1]
    rows = one.shape[0] // 8
    cols = head.shape[1] // 8
    half = o_tok.shape[0]

    def span(index, size):
        return pl.ds(pl.multiple_of(index * size, size), size)

    sources = [
        one.at[span(mine, rows), :],
        two.at[span(mine, rows), :],
        head.at[:, span(mine, cols)],
    ]
    places = [
        lambda side, q: o_one.at[span(q, rows), span(side, width)],
        lambda side, q: o_two.at[span(q, rows), span(side, width)],
        lambda side, q: o_head.at[side, :, span(q, cols)],
    ]

    greet([across, core, along, up])
    started = []

    def remote(src, dst, slot, target):
        copy = pltpu.make_async_remote_copy(
            src_ref=src,
            dst_ref=dst,
            send_sem=send.at[slot],
            recv_sem=recv.at[slot],
            device_id=target,
            device_id_type=MESH,
        )
        copy.start()
        started.append(copy)
        return copy

    firsts = [remote(sources[k], places[k](x, mine), 8 * k, across) for k in range(3)]
    extra = [
        remote(tok.at[span(other, half), :], o_tok.at[:, span(x, width)], 24, across),
        remote(tar.at[other], o_tar.at[x], 25, across),
    ]
    own = [
        pltpu.make_async_copy(one, o_one.at[:, span(x, width)], local.at[0]),
        pltpu.make_async_copy(two, o_two.at[:, span(x, width)], local.at[1]),
        pltpu.make_async_copy(head, o_head.at[x], local.at[2]),
        pltpu.make_async_copy(tok.at[span(x, half), :], o_tok.at[:, span(x, width)], local.at[3]),
        pltpu.make_async_copy(tar.at[x], o_tar.at[x], local.at[4]),
    ]
    for copy in own:
        copy.start()

    def pass_on(k, q, slot, target):
        piece = places[k](other, q)
        return remote(piece, piece, 8 * k + slot, target)

    ups, alongs, beyonds, ends = {}, {}, {}, []

    def stage_one(k):
        firsts[k].wait_recv()
        ups[k] = pass_on(k, mine, 1, up)
        alongs[k] = pass_on(k, mine, 2, along)
        ends.append(pass_on(k, mine, 4, core))

    def stage_two(k):
        ups[k].wait_recv()
        beyonds[k] = pass_on(k, flipped(mine, 2), 3, along)
        ends.append(pass_on(k, flipped(mine, 2), 5, core))

    def stage_three(k):
        alongs[k].wait_recv()
        ends.append(pass_on(k, flipped(mine, 1), 6, core))
        beyonds[k].wait_recv()
        ends.append(pass_on(k, flipped(flipped(mine, 1), 2), 7, core))

    stage_one(0)
    stage_one(1)
    stage_two(0)
    stage_one(2)
    stage_two(1)
    stage_two(2)
    for k in range(3):
        stage_three(k)
    for copy in ends + extra:
        copy.wait_recv()
    for copy in started:
        copy.wait_send()
    for copy in own:
        copy.wait()


def gather(tokens, first, second, head, targets):
    count, width = tokens.shape
    half = count // 2
    shape = jax.ShapeDtypeStruct
    return pl.pallas_call(
        gather_kernel,
        out_shape=(
            shape((half, 2 * width), tokens.dtype),
            shape((first.shape[0], 2 * first.shape[1]), first.dtype),
            shape((second.shape[0], 2 * second.shape[1]), second.dtype),
            shape((2,) + head.shape, head.dtype),
            shape(targets.shape, targets.dtype),
        ),
        in_specs=[VMEM] * 5,
        out_specs=[VMEM] * 5,
        scratch_shapes=[
            pltpu.SemaphoreType.DMA((26,)),
            pltpu.SemaphoreType.DMA((26,)),
            pltpu.SemaphoreType.DMA((5,)),
        ],
        compiler_params=params(0),
        name="gather",
    )(tokens, first, second, head, targets)


def total_kernel(groups, v_ref, o_ref, near, far, mid, send, recv):
    s, x = lax.axis_index("space"), lax.axis_index("tensor")
    low, high = s % 4, s // 4
    mine = x * 4 + low

    def near_peer(d):
        j = (mine + d) % 8
        return (high * 4 + j % 4, j // 4)

    def far_peer(d):
        return (((high + d) % groups) * 4 + low, x)

    greet([near_peer(d) for d in range(1, 8)] + [far_peer(d) for d in range(1, groups)])

    def share(src, slots, me, peers, base):
        copies = []
        for n, peer in enumerate(peers):
            copy = pltpu.make_async_remote_copy(
                src_ref=src,
                dst_ref=slots.at[me],
                send_sem=send.at[base + n],
                recv_sem=recv.at[base + n],
                device_id=peer,
                device_id_type=MESH,
            )
            copy.start()
            copies.append(copy)
        slots[me] = src[...]
        for copy in copies:
            copy.wait()

    share(v_ref, near, mine, [near_peer(d) for d in range(1, 8)], 0)
    mid[...] = jnp.sum(near[...], axis=0)
    share(mid, far, high, [far_peer(d) for d in range(1, groups)], 7)
    o_ref[...] = jnp.sum(far[...], axis=0)


def total(values):
    groups = lax.axis_size("space") // 4
    return pl.pallas_call(
        functools.partial(total_kernel, groups),
        out_shape=jax.ShapeDtypeStruct(values.shape, values.dtype),
        in_specs=[VMEM],
        out_specs=VMEM,
        scratch_shapes=[
            pltpu.VMEM((8,) + values.shape, values.dtype),
            pltpu.VMEM((groups,) + values.shape, values.dtype),
            pltpu.VMEM(values.shape, values.dtype),
            pltpu.SemaphoreType.DMA((6 + groups,)),
            pltpu.SemaphoreType.DMA((6 + groups,)),
        ],
        compiler_params=params(1),
        name="total",
    )(values)


X = -1


def orders(bits):
    rest = list(range(3, bits))
    return ([0, 1, 2, X] + rest, [0, 2, 1, X] + rest, [0, X, 1, 2] + rest)


def pieces(bits, order, shape):
    found = []
    left = list(range(bits))[::-1]
    rows, cols = shape
    for bit in order:
        if bit == X:
            cols //= 2
        else:
            left.remove(bit)
        found.append((2,) * len(left) + (rows, cols))
    return found


def scatter_kernel(bits, plan, *refs):
    grads, tok, refs = refs[:3], refs[3], refs[4:]
    outs, o_tok, refs = refs[:3], refs[3], refs[4:]
    count = bits + 1
    parts = len(plan)
    landing = [refs[count * k : count * (k + 1)] for k in range(parts)]
    refs = refs[parts * count :]
    away = [refs[bits * k : bits * (k + 1)] for k in range(parts)]
    refs = refs[parts * bits :]
    kept = [refs[bits * k : bits * (k + 1)] for k in range(parts)]
    send, recv = refs[parts * bits :]
    s, x = lax.axis_index("space"), lax.axis_index("tensor")

    def peer(bit):
        return (s, 1 - x) if bit == X else (flipped(s, bit), x)

    def part(ref, left, bit, near):
        if bit == X:
            width = ref.shape[-1] // 2
            side = x if near else 1 - x
            place = pl.ds(pl.multiple_of(side * width, width), width)
            return (slice(None),) * (len(ref.shape) - 1) + (place,)
        value = (s // (1 << bit)) % 2
        value = value if near else 1 - value
        return (slice(None),) * left.index(bit) + (value,)

    greet([peer(b) for b in [X] + list(range(bits))])
    copies = []

    def start(k, n, src):
        copy = pltpu.make_async_remote_copy(
            src_ref=src,
            dst_ref=landing[k][n],
            send_sem=send.at[k * count + n],
            recv_sem=recv.at[k * count + n],
            device_id=peer(plan[k][3][n]),
            device_id_type=MESH,
        )
        copy.start()
        copies.append(copy)
        return copy

    state = []
    for k, (which, first, rows, order) in enumerate(plan):
        left = list(range(bits))[::-1]
        ref = grads[which].at[(slice(None),) * bits + (pl.ds(first, rows),)]
        copy = start(k, 0, ref.at[part(ref, left, order[0], False)])
        left_now = [b for b in left if b != order[0]]
        state.append((ref.at[part(ref, left, order[0], True)], left_now, copy))
    width = tok.shape[1] // 2
    tail = pltpu.make_async_remote_copy(
        src_ref=tok.at[:, pl.ds(pl.multiple_of((1 - x) * width, width), width)],
        dst_ref=o_tok,
        send_sem=send.at[parts * count],
        recv_sem=recv.at[parts * count],
        device_id=peer(X),
        device_id_type=MESH,
    )
    tail.start()
    copies.append(tail)

    def added(ref, arrived, index):
        return ref[index].astype(jnp.float32) + arrived[index].astype(jnp.float32)

    for n in range(count):
        for k, (which, first, rows, order) in enumerate(plan):
            ref, left, copy = state[k]
            arrived = landing[k][n]
            copy.wait_recv()
            if n == count - 1:
                outs[which][pl.ds(first, rows), :] = added(ref, arrived, ...)
                continue
            bit = order[n + 1]
            far = away[k][n]
            far[...] = added(ref, arrived, part(arrived, left, bit, False)).astype(far.dtype)
            copy = start(k, n + 1, far)
            near = kept[k][n]
            near[...] = added(ref, arrived, part(arrived, left, bit, True))
            state[k] = (near, [b for b in left if b != bit], copy)
    tail.wait_recv()
    for copy in copies:
        copy.wait_send()


def scatter(g_one, g_two, g_head, tok):
    size = lax.axis_size("space")
    bits = size.bit_length() - 1
    steps = orders(bits)
    grads = [g.reshape((2,) * bits + (g.shape[0] // size, g.shape[1])) for g in (g_one, g_two, g_head)]
    rows = grads[0].shape[-2]
    half = rows // 2
    plan = [
        (0, 0, half, steps[0]),
        (1, 0, half, steps[1]),
        (2, 0, rows, steps[2]),
        (0, half, half, steps[0]),
        (1, half, half, steps[1]),
    ]
    shapes = [pieces(bits, order, (n, grads[which].shape[-1])) for which, _, n, order in plan]
    scratch = [pltpu.VMEM(shape, jnp.bfloat16) for found in shapes for shape in found]
    scratch += [pltpu.VMEM(shape, jnp.bfloat16) for found in shapes for shape in found[1:]]
    scratch += [pltpu.VMEM(shape, jnp.float32) for found in shapes for shape in found[1:]]
    slots = len(plan) * (bits + 1) + 1
    outs = [shapes[which][-1][-1] for which in range(3)]
    return pl.pallas_call(
        functools.partial(scatter_kernel, bits, plan),
        out_shape=tuple(jax.ShapeDtypeStruct((rows, width), jnp.float32) for width in outs)
        + (jax.ShapeDtypeStruct((tok.shape[0], tok.shape[1] // 2), tok.dtype),),
        in_specs=[VMEM] * 4,
        out_specs=[VMEM] * 4,
        scratch_shapes=scratch
        + [pltpu.SemaphoreType.DMA((slots,)), pltpu.SemaphoreType.DMA((slots,))],
        compiler_params=params(2),
        name="scatter",
    )(*grads, tok)


def mix(a, b, dims):
    return lax.dot_general(a, b, ((dims[:1], dims[1:]), ((), ())), preferred_element_type=jnp.float32)


def per_device(
    tokens, first_weight, second_weight, head_weight, targets, land_mask, variable_kind, loss_scale
):
    low = jnp.bfloat16
    count, width = tokens.shape
    half = count // 2
    rows = head_weight.shape[0]
    kinds = 2 * rows // PP
    s, x = lax.axis_index("space"), lax.axis_index("tensor")
    lanes = -(-(half + 1) // 128) * 128
    sent = jnp.stack([targets[:, :half], targets[:, half:]]).astype(low)
    label = jnp.repeat(variable_kind, PP).astype(low)[None, :, None]
    label = jnp.broadcast_to(label, (2, rows, lanes - half))
    sent = jnp.concatenate([sent, label], axis=2)
    toks, w_one, w_two, w_head, seen = gather(
        tokens, first_weight, second_weight, head_weight, sent
    )
    w_head = w_head.reshape(2 * rows, -1)
    goal = seen[:, :, :half].reshape(kinds, PP, half)
    kind = seen[:, :, half].reshape(kinds, PP)[:, :, None]

    position = s * count + x * half + jnp.arange(half, dtype=jnp.int32)
    cell = jnp.arange(PP, dtype=jnp.int32)
    lat_row = 2 * (position // LONP)[None, :] + (cell // 2)[:, None]
    nlat = 2 * PROW_DEV * lax.axis_size("space")
    cell_weight = jnp.cos(math.pi / 2.0 * (lat_row.astype(jnp.float32) + 0.5) / nlat)
    land = lax.dynamic_slice_in_dim(land_mask, x * half, half, 1).astype(jnp.float32)
    valid = jnp.where(kind == 0, 1.0, jnp.where(kind == 1, land[None], 1.0 - land[None]))
    masked = cell_weight[None] * valid

    pre_one = mix(toks, w_one, (1, 0))
    hidden_one = bent(pre_one)
    pre_two = mix(hidden_one, w_two, (1, 0))
    hidden_two = bent(pre_two)
    predicted = mix(w_head, hidden_two, (1, 1))
    error = predicted.reshape(kinds, PP, half) - goal.astype(jnp.float32)
    scored = masked * error
    sums = jnp.stack([jnp.sum(scored * error, axis=(1, 2)), jnp.sum(masked, axis=(1, 2))])
    wide = -(-kinds // 128) * 128
    sums = total(jnp.pad(sums, ((0, 6), (0, wide - kinds))))
    weight_sum = sums[1, :kinds]
    root = jnp.sqrt(sums[0, :kinds] / weight_sum + 1e-06)
    loss = jnp.sum(root) / kinds
    coef = loss_scale / (kinds * root * weight_sum)
    grad_pred = (coef[:, None, None] * scored).reshape(kinds * PP, half).astype(low)

    head_term = mix(hidden_two, grad_pred, (0, 1)).astype(low)
    pad = jnp.zeros((head_term.shape[0], -rows % 128), low)
    head_term = jnp.concatenate([head_term[:, :rows], pad, head_term[:, rows:], pad], axis=1)
    grad_two = (mix(grad_pred, w_head, (0, 0)) * slope(pre_two)).astype(low)
    second_term = mix(hidden_one, grad_two, (0, 0)).astype(low)
    grad_one = (mix(grad_two, w_two, (1, 1)) * slope(pre_one)).astype(low)
    first_term = mix(toks, grad_one, (0, 0)).astype(low)
    token_term = mix(grad_one, w_one, (1, 1)).astype(low)
    first_grad, second_grad, head_grad, arrived = scatter(
        first_term, second_term, head_term, token_term
    )
    kept = lax.dynamic_slice_in_dim(token_term, x * width, width, 1)
    side = lax.broadcasted_iota(jnp.int32, (2, half, width), 0)
    token_grad = jnp.where(side == x, kept[None], arrived[None]).astype(jnp.float32)
    token_grad = token_grad.reshape(count, width)
    return (loss, token_grad, first_grad, second_grad, head_grad[:, :rows].T)


def column_folder(weights, piece):
    return lax.dot_general(
        piece, weights, (((1,), (1,)), ((), ())), preferred_element_type=jnp.float32
    )


def row_folder(weights, piece):
    return lax.dot_general(
        piece, weights, (((0,), (0,)), ((), ())), preferred_element_type=jnp.float32
    )


def per_device_wide(
    tokens, first_weight, second_weight, head_weight, targets, land_mask, variable_kind, loss_scale
):
    count = tokens.shape[0]
    width = first_weight.shape[1]
    kinds = head_weight.shape[0] // PP
    rows_first, rows_second = (
        lax.all_to_all(first_weight, "tensor", split_axis=0, concat_axis=1, tiled=True),
        lax.all_to_all(second_weight, "tensor", split_axis=0, concat_axis=1, tiled=True),
    )
    head_cols = lax.all_to_all(head_weight, "tensor", split_axis=1, concat_axis=0, tiled=True)
    position = lax.axis_index("space") * count + jnp.arange(count, dtype=jnp.int32)
    cell = jnp.arange(PP, dtype=jnp.int32)
    lat_row = 2 * (position // LONP)[None, :] + (cell // 2)[:, None]
    nlat = 2 * PROW_DEV * lax.axis_size("space")
    cell_weight = jnp.cos(math.pi / 2.0 * (lat_row.astype(jnp.float32) + 0.5) / nlat)
    land = land_mask.astype(jnp.float32)
    kind = variable_kind[:, None, None]
    valid = jnp.where(kind == 0, 1.0, jnp.where(kind == 1, land[None], 1.0 - land[None]))
    masked = cell_weight[None] * valid
    local_weight = jnp.sum(masked, axis=(1, 2))
    weight_sum = lax.psum(local_weight, "space")
    full_in = lax.all_gather(tokens, "tensor", axis=1, tiled=True)
    pre_one = jnp.dot(full_in, first_weight, preferred_element_type=jnp.float32)
    hidden_one = jax.nn.gelu(pre_one, approximate=False).astype(jnp.bfloat16)
    full_one = lax.all_gather(hidden_one, "tensor", axis=1, tiled=True)
    pre_two = jnp.dot(full_one, second_weight, preferred_element_type=jnp.float32)
    hidden_two = jax.nn.gelu(pre_two, approximate=False).astype(jnp.bfloat16)
    full_two = lax.all_gather(hidden_two, "tensor", axis=1, tiled=True)
    predicted = lax.dot_general(
        head_weight, full_two, (((1,), (1,)), ((), ())), preferred_element_type=jnp.float32
    )
    error = predicted.reshape(kinds, PP, count) - targets.reshape(kinds, PP, count)
    local_error = jnp.sum(masked * error * error, axis=(1, 2))
    error_sum = lax.psum(local_error, "space")
    root = jnp.sqrt(error_sum / weight_sum + 1e-06)
    loss = lax.psum(jnp.sum(root), "tensor") / (kinds * lax.axis_size("tensor"))
    coef = loss_scale / (kinds * lax.axis_size("tensor") * root * weight_sum)
    grad_pred = (
        (coef[:, None, None] * masked * error).reshape(kinds * PP, count).astype(jnp.bfloat16)
    )
    back_two = row_folder(head_cols, lax.all_gather(grad_pred, "tensor", axis=0, tiled=True))
    head_term = jnp.dot(grad_pred, full_two, preferred_element_type=jnp.float32)
    head_grad = lax.psum_scatter(head_term, "space", scatter_dimension=1, tiled=True)
    grad_two = (back_two * slope(pre_two)).astype(jnp.bfloat16)
    back_one = column_folder(rows_second, lax.all_gather(grad_two, "tensor", axis=1, tiled=True))
    grad_one = (back_one * slope(pre_one)).astype(jnp.bfloat16)
    joined = lax.psum_scatter(
        jnp.concatenate(
            [
                lax.dot_general(
                    full_one, grad_two, (((0,), (0,)), ((), ())), preferred_element_type=jnp.float32
                ),
                lax.dot_general(
                    full_in, grad_one, (((0,), (0,)), ((), ())), preferred_element_type=jnp.float32
                ),
            ],
            axis=1,
        ),
        "space",
        scatter_dimension=0,
        tiled=True,
    )
    second_grad = joined[:, :width]
    first_grad = joined[:, width:]
    token_grad = column_folder(rows_first, lax.all_gather(grad_one, "tensor", axis=1, tiled=True))
    return (loss, token_grad, first_grad, second_grad, head_grad)


def solution(mesh):
    size = mesh.shape["space"]
    paired = mesh.shape["tensor"] == 2 and size >= 8 and size & (size - 1) == 0
    return jax.shard_map(
        per_device if paired else per_device_wide,
        mesh=mesh,
        in_specs=(
            P("space", "tensor"),
            P(None, "tensor"),
            P(None, "tensor"),
            P("tensor", None),
            P("tensor", "space"),
            P(None, "space"),
            P("tensor"),
            P(),
        ),
        out_specs=(
            P(),
            P("space", "tensor"),
            P("space", "tensor"),
            P("space", "tensor"),
            P("tensor", "space"),
        ),
        check_vma=False,
    )
```

```python
import functools
import math

import jax
import jax.numpy as jnp
from jax import lax
from jax.experimental import pallas as pl
from jax.experimental.pallas import tpu as pltpu
from jax.sharding import PartitionSpec as P

PP = 4
PROW_DEV = 4
LONP = 224
MESH = pl.DeviceIdType.MESH
VMEM = pl.BlockSpec(memory_space=pltpu.VMEM)
ANY = pl.BlockSpec(memory_space=pl.ANY)


def bent(z):
    return (0.5 * z * (1.0 + lax.erf(z / math.sqrt(2.0)))).astype(jnp.bfloat16)


def slope(z):
    cdf = 0.5 * (1.0 + lax.erf(z / math.sqrt(2.0)))
    return cdf + z * jnp.exp(-0.5 * z * z) / math.sqrt(2.0 * math.pi)


def flipped(s, bit):
    step = 1 << bit
    return s + step - 2 * step * ((s // step) % 2)


def greet(partners):
    barrier = pltpu.get_barrier_semaphore()
    for partner in partners:
        pl.semaphore_signal(barrier, inc=1, device_id=partner, device_id_type=MESH)
    pl.semaphore_wait(barrier, len(partners))


def params(number, mib):
    return pltpu.CompilerParams(
        collective_id=number, has_side_effects=True, vmem_limit_bytes=mib * 2**20
    )


def gather_kernel(
    tok, one, two, head, tar, o_tok, o_one, o_two, o_head, o_tar, h_one, h_two, h_head, h_tok, h_tar, send, recv, local
):
    s, x = lax.axis_index("space"), lax.axis_index("tensor")
    other = 1 - x
    across, core, along, up = (s, other), (flipped(s, 0), x), (flipped(s, 1), x), (flipped(s, 2), x)
    mine = s % 8
    width = one.shape[1]
    rows = one.shape[0] // 8
    cols = head.shape[1] // 8
    half = o_tok.shape[0]

    def span(index, size):
        return pl.ds(pl.multiple_of(index * size, size), size)

    sources = [
        one.at[span(mine, rows), :],
        two.at[span(mine, rows), :],
        head.at[:, span(mine, cols)],
    ]
    places = [
        lambda side, q: o_one.at[span(q, rows), span(side, width)],
        lambda side, q: o_two.at[span(q, rows), span(side, width)],
        lambda side, q: o_head.at[side, :, span(q, cols)],
    ]

    greet([across, core, along, up])
    started = []

    def remote(src, dst, slot, target):
        copy = pltpu.make_async_remote_copy(
            src_ref=src,
            dst_ref=dst,
            send_sem=send.at[slot],
            recv_sem=recv.at[slot],
            device_id=target,
            device_id_type=MESH,
        )
        copy.start()
        started.append(copy)
        return copy

    firsts = [remote(sources[k], places[k](x, mine), 8 * k, across) for k in range(3)]
    extra = [
        remote(tok.at[span(other, half), :], o_tok.at[:, span(x, width)], 24, across),
        remote(tar.at[other], o_tar.at[x], 25, across),
    ]
    moves = [
        (one, h_one, o_one.at[:, span(x, width)]),
        (two, h_two, o_two.at[:, span(x, width)]),
        (head, h_head, o_head.at[x]),
        (tok.at[span(x, half), :], h_tok, o_tok.at[:, span(x, width)]),
        (tar.at[x], h_tar, o_tar.at[x]),
    ]
    held = [pltpu.make_async_copy(a, b, local.at[n]) for n, (a, b, _) in enumerate(moves)]
    own = [pltpu.make_async_copy(b, c, local.at[5 + n]) for n, (_, b, c) in enumerate(moves)]
    for copy in held:
        copy.start()
    for first, second in zip(held, own):
        first.wait()
        second.start()

    def pass_on(k, q, slot, target):
        piece = places[k](other, q)
        return remote(piece, piece, 8 * k + slot, target)

    ups, alongs, beyonds, ends = {}, {}, {}, []

    def stage_one(k):
        firsts[k].wait_recv()
        ups[k] = pass_on(k, mine, 1, up)
        alongs[k] = pass_on(k, mine, 2, along)
        ends.append(pass_on(k, mine, 4, core))

    def stage_two(k):
        ups[k].wait_recv()
        beyonds[k] = pass_on(k, flipped(mine, 2), 3, along)
        ends.append(pass_on(k, flipped(mine, 2), 5, core))

    def stage_three(k):
        alongs[k].wait_recv()
        ends.append(pass_on(k, flipped(mine, 1), 6, core))
        beyonds[k].wait_recv()
        ends.append(pass_on(k, flipped(flipped(mine, 1), 2), 7, core))

    stage_one(0)
    stage_one(1)
    stage_two(0)
    stage_one(2)
    stage_two(1)
    stage_two(2)
    for k in range(3):
        stage_three(k)
    for copy in ends + extra:
        copy.wait_recv()
    for copy in started:
        copy.wait_send()
    for copy in own:
        copy.wait()


def gather(tokens, first, second, head, targets):
    count, width = tokens.shape
    half = count // 2
    shape = jax.ShapeDtypeStruct
    return pl.pallas_call(
        gather_kernel,
        out_shape=(
            shape((half, 2 * width), tokens.dtype),
            shape((first.shape[0], 2 * first.shape[1]), first.dtype),
            shape((second.shape[0], 2 * second.shape[1]), second.dtype),
            shape((2,) + head.shape, head.dtype),
            shape(targets.shape, targets.dtype),
        ),
        in_specs=[ANY] * 5,
        out_specs=[ANY] * 5,
        scratch_shapes=[
            pltpu.VMEM(first.shape, first.dtype),
            pltpu.VMEM(second.shape, second.dtype),
            pltpu.VMEM(head.shape, head.dtype),
            pltpu.VMEM((half, width), tokens.dtype),
            pltpu.VMEM(targets.shape[1:], targets.dtype),
            pltpu.SemaphoreType.DMA((26,)),
            pltpu.SemaphoreType.DMA((26,)),
            pltpu.SemaphoreType.DMA((10,)),
        ],
        compiler_params=params(0, 16),
        name="gather",
    )(tokens, first, second, head, targets)


def total_kernel(groups, v_ref, o_ref, near, far, mid, send, recv):
    s, x = lax.axis_index("space"), lax.axis_index("tensor")
    low, high = s % 4, s // 4
    mine = x * 4 + low

    def near_peer(d):
        j = (mine + d) % 8
        return (high * 4 + j % 4, j // 4)

    def far_peer(d):
        return (((high + d) % groups) * 4 + low, x)

    greet([near_peer(d) for d in range(1, 8)] + [far_peer(d) for d in range(1, groups)])

    def share(src, slots, me, peers, base):
        copies = []
        for n, peer in enumerate(peers):
            copy = pltpu.make_async_remote_copy(
                src_ref=src,
                dst_ref=slots.at[me],
                send_sem=send.at[base + n],
                recv_sem=recv.at[base + n],
                device_id=peer,
                device_id_type=MESH,
            )
            copy.start()
            copies.append(copy)
        slots[me] = src[...]
        for copy in copies:
            copy.wait()

    share(v_ref, near, mine, [near_peer(d) for d in range(1, 8)], 0)
    mid[...] = jnp.sum(near[...], axis=0)
    share(mid, far, high, [far_peer(d) for d in range(1, groups)], 7)
    o_ref[...] = jnp.sum(far[...], axis=0)


def total(values):
    groups = lax.axis_size("space") // 4
    return pl.pallas_call(
        functools.partial(total_kernel, groups),
        out_shape=jax.ShapeDtypeStruct(values.shape, values.dtype),
        in_specs=[VMEM],
        out_specs=VMEM,
        scratch_shapes=[
            pltpu.VMEM((8,) + values.shape, values.dtype),
            pltpu.VMEM((groups,) + values.shape, values.dtype),
            pltpu.VMEM(values.shape, values.dtype),
            pltpu.SemaphoreType.DMA((6 + groups,)),
            pltpu.SemaphoreType.DMA((6 + groups,)),
        ],
        compiler_params=params(1, 4),
        name="total",
    )(values)


X = -1


def orders(bits):
    rest = list(range(3, bits))
    return ([0, 1, 2, X] + rest, [0, 2, 1, X] + rest, [0, X, 1, 2] + rest)


def pieces(bits, order, shape):
    found = []
    left = list(range(bits))[::-1]
    rows, cols = shape
    for bit in order:
        if bit == X:
            cols //= 2
        else:
            left.remove(bit)
        found.append((2,) * len(left) + (rows, cols))
    return found


def scatter_kernel(bits, plan, *refs):
    grads, tok, refs = refs[:3], refs[3], refs[4:]
    outs, o_tok, refs = refs[:3], refs[3], refs[4:]
    count = bits + 1
    parts = len(plan)
    landing = [refs[count * k : count * (k + 1)] for k in range(parts)]
    refs = refs[parts * count :]
    away = [refs[bits * k : bits * (k + 1)] for k in range(parts)]
    refs = refs[parts * bits :]
    kept = [refs[bits * k : bits * (k + 1)] for k in range(parts)]
    refs = refs[parts * bits :]
    near_in = refs[:parts]
    send, recv, local = refs[parts:]
    s, x = lax.axis_index("space"), lax.axis_index("tensor")

    def peer(bit):
        return (s, 1 - x) if bit == X else (flipped(s, bit), x)

    def part(ref, left, bit, near):
        if bit == X:
            width = ref.shape[-1] // 2
            side = x if near else 1 - x
            place = pl.ds(pl.multiple_of(side * width, width), width)
            return (slice(None),) * (len(ref.shape) - 1) + (place,)
        value = (s // (1 << bit)) % 2
        value = value if near else 1 - value
        return (slice(None),) * left.index(bit) + (value,)

    greet([peer(b) for b in [X] + list(range(bits))])
    copies = []

    def start(k, n, src):
        copy = pltpu.make_async_remote_copy(
            src_ref=src,
            dst_ref=landing[k][n],
            send_sem=send.at[k * count + n],
            recv_sem=recv.at[k * count + n],
            device_id=peer(plan[k][3][n]),
            device_id_type=MESH,
        )
        copy.start()
        copies.append(copy)
        return copy

    state = []
    for k, (which, first, rows, order) in enumerate(plan):
        left = list(range(bits))[::-1]
        ref = grads[which].at[(slice(None),) * bits + (pl.ds(first, rows),)]
        copy = start(k, 0, ref.at[part(ref, left, order[0], False)])
        left_now = [b for b in left if b != order[0]]
        state.append((ref.at[part(ref, left, order[0], True)], left_now, copy))
    inner = []
    for k in range(parts):
        ref, left, copy = state[k]
        inner.append(pltpu.make_async_copy(ref, near_in[k], local.at[k]))
        inner[k].start()
        state[k] = (near_in[k], left, copy)
    width = tok.shape[1] // 2
    tail = pltpu.make_async_remote_copy(
        src_ref=tok.at[:, pl.ds(pl.multiple_of((1 - x) * width, width), width)],
        dst_ref=o_tok,
        send_sem=send.at[parts * count],
        recv_sem=recv.at[parts * count],
        device_id=peer(X),
        device_id_type=MESH,
    )
    tail.start()
    copies.append(tail)

    def added(ref, arrived, index):
        return ref[index].astype(jnp.float32) + arrived[index].astype(jnp.float32)

    for n in range(count):
        for k, (which, first, rows, order) in enumerate(plan):
            ref, left, copy = state[k]
            arrived = landing[k][n]
            copy.wait_recv()
            if n == 0:
                inner[k].wait()
            if n == count - 1:
                outs[which][pl.ds(first, rows), :] = added(ref, arrived, ...)
                continue
            bit = order[n + 1]
            far = away[k][n]
            far[...] = added(ref, arrived, part(arrived, left, bit, False)).astype(far.dtype)
            copy = start(k, n + 1, far)
            near = kept[k][n]
            near[...] = added(ref, arrived, part(arrived, left, bit, True))
            state[k] = (near, [b for b in left if b != bit], copy)
    tail.wait_recv()
    for copy in copies:
        copy.wait_send()


def scatter(g_one, g_two, g_head, tok):
    size = lax.axis_size("space")
    bits = size.bit_length() - 1
    steps = orders(bits)
    grads = [g.reshape((2,) * bits + (g.shape[0] // size, g.shape[1])) for g in (g_one, g_two, g_head)]
    rows = grads[0].shape[-2]
    half = rows // 2
    plan = [
        (0, 0, half, steps[0]),
        (1, 0, half, steps[1]),
        (2, 0, rows, steps[2]),
        (0, half, half, steps[0]),
        (1, half, half, steps[1]),
    ]
    shapes = [pieces(bits, order, (n, grads[which].shape[-1])) for which, _, n, order in plan]
    scratch = [pltpu.VMEM(shape, jnp.bfloat16) for found in shapes for shape in found]
    scratch += [pltpu.VMEM(shape, jnp.bfloat16) for found in shapes for shape in found[1:]]
    scratch += [pltpu.VMEM(shape, jnp.float32) for found in shapes for shape in found[1:]]
    scratch += [pltpu.VMEM(found[0], jnp.bfloat16) for found in shapes]
    slots = len(plan) * (bits + 1) + 1
    outs = [shapes[which][-1][-1] for which in range(3)]
    return pl.pallas_call(
        functools.partial(scatter_kernel, bits, plan),
        out_shape=tuple(jax.ShapeDtypeStruct((rows, width), jnp.float32) for width in outs)
        + (jax.ShapeDtypeStruct((tok.shape[0], tok.shape[1] // 2), tok.dtype),),
        in_specs=[ANY] * 4,
        out_specs=[VMEM] * 3 + [ANY],
        scratch_shapes=scratch
        + [pltpu.SemaphoreType.DMA((n,)) for n in (slots, slots, len(plan))],
        compiler_params=params(2, 28),
        name="scatter",
    )(*grads, tok)


def mix(a, b, dims):
    return lax.dot_general(a, b, ((dims[:1], dims[1:]), ((), ())), preferred_element_type=jnp.float32)


def per_device(
    tokens, first_weight, second_weight, head_weight, targets, land_mask, variable_kind, loss_scale
):
    low = jnp.bfloat16
    count, width = tokens.shape
    half = count // 2
    rows = head_weight.shape[0]
    kinds = 2 * rows // PP
    s, x = lax.axis_index("space"), lax.axis_index("tensor")
    lanes = -(-(half + 1) // 128) * 128
    sent = jnp.stack([targets[:, :half], targets[:, half:]]).astype(low)
    label = jnp.repeat(variable_kind, PP).astype(low)[None, :, None]
    label = jnp.broadcast_to(label, (2, rows, lanes - half))
    sent = jnp.concatenate([sent, label], axis=2)
    toks, w_one, w_two, w_head, seen = gather(
        tokens, first_weight, second_weight, head_weight, sent
    )
    w_head = w_head.reshape(2 * rows, -1)
    goal = seen[:, :, :half].reshape(kinds, PP, half)
    kind = seen[:, :, half].reshape(kinds, PP)[:, :, None]

    position = s * count + x * half + jnp.arange(half, dtype=jnp.int32)
    cell = jnp.arange(PP, dtype=jnp.int32)
    lat_row = 2 * (position // LONP)[None, :] + (cell // 2)[:, None]
    nlat = 2 * PROW_DEV * lax.axis_size("space")
    cell_weight = jnp.cos(math.pi / 2.0 * (lat_row.astype(jnp.float32) + 0.5) / nlat)
    land = lax.dynamic_slice_in_dim(land_mask, x * half, half, 1).astype(jnp.float32)
    valid = jnp.where(kind == 0, 1.0, jnp.where(kind == 1, land[None], 1.0 - land[None]))
    masked = cell_weight[None] * valid

    pre_one = mix(toks, w_one, (1, 0))
    hidden_one = bent(pre_one)
    pre_two = mix(hidden_one, w_two, (1, 0))
    hidden_two = bent(pre_two)
    predicted = mix(w_head, hidden_two, (1, 1))
    error = predicted.reshape(kinds, PP, half) - goal.astype(jnp.float32)
    scored = masked * error
    sums = jnp.stack([jnp.sum(scored * error, axis=(1, 2)), jnp.sum(masked, axis=(1, 2))])
    wide = -(-kinds // 128) * 128
    sums = total(jnp.pad(sums, ((0, 6), (0, wide - kinds))))
    weight_sum = sums[1, :kinds]
    root = jnp.sqrt(sums[0, :kinds] / weight_sum + 1e-06)
    loss = jnp.sum(root) / kinds
    coef = loss_scale / (kinds * root * weight_sum)
    grad_pred = (coef[:, None, None] * scored).reshape(kinds * PP, half).astype(low)

    head_term = mix(hidden_two, grad_pred, (0, 1)).astype(low)
    pad = jnp.zeros((head_term.shape[0], -rows % 128), low)
    head_term = jnp.concatenate([head_term[:, :rows], pad, head_term[:, rows:], pad], axis=1)
    grad_two = (mix(grad_pred, w_head, (0, 0)) * slope(pre_two)).astype(low)
    second_term = mix(hidden_one, grad_two, (0, 0)).astype(low)
    grad_one = (mix(grad_two, w_two, (1, 1)) * slope(pre_one)).astype(low)
    first_term = mix(toks, grad_one, (0, 0)).astype(low)
    token_term = mix(grad_one, w_one, (1, 1)).astype(low)
    first_grad, second_grad, head_grad, arrived = scatter(
        first_term, second_term, head_term, token_term
    )
    kept = lax.dynamic_slice_in_dim(token_term, x * width, width, 1)
    side = lax.broadcasted_iota(jnp.int32, (2, half, width), 0)
    token_grad = jnp.where(side == x, kept[None], arrived[None]).astype(jnp.float32)
    token_grad = token_grad.reshape(count, width)
    return (loss, token_grad, first_grad, second_grad, head_grad[:, :rows].T)


def column_folder(weights, piece):
    return lax.dot_general(
        piece, weights, (((1,), (1,)), ((), ())), preferred_element_type=jnp.float32
    )


def row_folder(weights, piece):
    return lax.dot_general(
        piece, weights, (((0,), (0,)), ((), ())), preferred_element_type=jnp.float32
    )


def per_device_wide(
    tokens, first_weight, second_weight, head_weight, targets, land_mask, variable_kind, loss_scale
):
    count = tokens.shape[0]
    width = first_weight.shape[1]
    kinds = head_weight.shape[0] // PP
    rows_first, rows_second = (
        lax.all_to_all(first_weight, "tensor", split_axis=0, concat_axis=1, tiled=True),
        lax.all_to_all(second_weight, "tensor", split_axis=0, concat_axis=1, tiled=True),
    )
    head_cols = lax.all_to_all(head_weight, "tensor", split_axis=1, concat_axis=0, tiled=True)
    position = lax.axis_index("space") * count + jnp.arange(count, dtype=jnp.int32)
    cell = jnp.arange(PP, dtype=jnp.int32)
    lat_row = 2 * (position // LONP)[None, :] + (cell // 2)[:, None]
    nlat = 2 * PROW_DEV * lax.axis_size("space")
    cell_weight = jnp.cos(math.pi / 2.0 * (lat_row.astype(jnp.float32) + 0.5) / nlat)
    land = land_mask.astype(jnp.float32)
    kind = variable_kind[:, None, None]
    valid = jnp.where(kind == 0, 1.0, jnp.where(kind == 1, land[None], 1.0 - land[None]))
    masked = cell_weight[None] * valid
    local_weight = jnp.sum(masked, axis=(1, 2))
    weight_sum = lax.psum(local_weight, "space")
    full_in = lax.all_gather(tokens, "tensor", axis=1, tiled=True)
    pre_one = jnp.dot(full_in, first_weight, preferred_element_type=jnp.float32)
    hidden_one = jax.nn.gelu(pre_one, approximate=False).astype(jnp.bfloat16)
    full_one = lax.all_gather(hidden_one, "tensor", axis=1, tiled=True)
    pre_two = jnp.dot(full_one, second_weight, preferred_element_type=jnp.float32)
    hidden_two = jax.nn.gelu(pre_two, approximate=False).astype(jnp.bfloat16)
    full_two = lax.all_gather(hidden_two, "tensor", axis=1, tiled=True)
    predicted = lax.dot_general(
        head_weight, full_two, (((1,), (1,)), ((), ())), preferred_element_type=jnp.float32
    )
    error = predicted.reshape(kinds, PP, count) - targets.reshape(kinds, PP, count)
    local_error = jnp.sum(masked * error * error, axis=(1, 2))
    error_sum = lax.psum(local_error, "space")
    root = jnp.sqrt(error_sum / weight_sum + 1e-06)
    loss = lax.psum(jnp.sum(root), "tensor") / (kinds * lax.axis_size("tensor"))
    coef = loss_scale / (kinds * lax.axis_size("tensor") * root * weight_sum)
    grad_pred = (
        (coef[:, None, None] * masked * error).reshape(kinds * PP, count).astype(jnp.bfloat16)
    )
    back_two = row_folder(head_cols, lax.all_gather(grad_pred, "tensor", axis=0, tiled=True))
    head_term = jnp.dot(grad_pred, full_two, preferred_element_type=jnp.float32)
    head_grad = lax.psum_scatter(head_term, "space", scatter_dimension=1, tiled=True)
    grad_two = (back_two * slope(pre_two)).astype(jnp.bfloat16)
    back_one = column_folder(rows_second, lax.all_gather(grad_two, "tensor", axis=1, tiled=True))
    grad_one = (back_one * slope(pre_one)).astype(jnp.bfloat16)
    joined = lax.psum_scatter(
        jnp.concatenate(
            [
                lax.dot_general(
                    full_one, grad_two, (((0,), (0,)), ((), ())), preferred_element_type=jnp.float32
                ),
                lax.dot_general(
                    full_in, grad_one, (((0,), (0,)), ((), ())), preferred_element_type=jnp.float32
                ),
            ],
            axis=1,
        ),
        "space",
        scatter_dimension=0,
        tiled=True,
    )
    second_grad = joined[:, :width]
    first_grad = joined[:, width:]
    token_grad = column_folder(rows_first, lax.all_gather(grad_one, "tensor", axis=1, tiled=True))
    return (loss, token_grad, first_grad, second_grad, head_grad)


def solution(mesh):
    size = mesh.shape["space"]
    paired = mesh.shape["tensor"] == 2 and size >= 8 and size & (size - 1) == 0
    return jax.shard_map(
        per_device if paired else per_device_wide,
        mesh=mesh,
        in_specs=(
            P("space", "tensor"),
            P(None, "tensor"),
            P(None, "tensor"),
            P("tensor", None),
            P("tensor", "space"),
            P(None, "space"),
            P("tensor"),
            P(),
        ),
        out_specs=(
            P(),
            P("space", "tensor"),
            P("space", "tensor"),
            P("space", "tensor"),
            P("tensor", "space"),
        ),
        check_vma=False,
    )
```
